32 devices in a mesh: wide: 8 (over z, x), narrow: 4 (over y, core).
Axes of the slice: x: 2, y: 2, z: 4, core: 2. Of those that a mesh axis runs over, the one named last changes fastest.
Arguments:
- old_basis: float32 [16, 2048, 512], P(None, ('wide', 'narrow')), may hold values from -6 to 6
- restart_coeffs: float32 [16], replicated, may hold values from -1 to 1
- geometry: float32 [4, 2048, 512], P(None, ('wide', 'narrow')), may hold values from 0.01 to 18, as said below
- orientation: int32 [6, 2048], P(None, ('wide', 'narrow')), may hold values from 0 to 7
Outputs:
- new_basis: float32 [2, 2048, 512], P(None, ('wide', 'narrow'))
- hessenberg: float32 [2, 18], replicated
The draws below stay inside these ranges and needn't reach their ends.
Inputs may be any that keep to these rules, and one draw needn't show every extreme that they name: `geometry`: every entry is positive.
All inputs are finite; a program needn't handle non-finite values.
Results may differ from the reference program's by a relative error of at most 0.0003.
Values sent between devices are 32-bit elements; how exact they have to be, the bound alone decides.
A program may use at most 64 MiB of HBM per device.

```python
import jax
import jax.numpy as jnp
import numpy as np
from jax import lax

NP = 8
PTS = 512
KB = 16
EX = 4
EY = 4
EZ = 4
ELEMS = 2048
N_WIDE = 8
N_NARROW = 4


def draw_geometry(key, part):
    noise = jax.random.uniform(jax.random.fold_in(key, 17), (4, ELEMS, PTS), jnp.float32)
    lower = jnp.array([0.01, 0.01, 0.01, 0.5], jnp.float32).reshape(4, 1, 1)
    upper = jnp.array([0.04, 0.04, 0.04, 2.0], jnp.float32).reshape(4, 1, 1)
    position = jnp.arange(ELEMS, dtype=jnp.float32) / max(ELEMS - 1, 1)
    base_vals = jnp.exp(jnp.log(lower) + noise * (jnp.log(upper) - jnp.log(lower)))
    ramp_vals = 1.0 + 2.0 * position
    return (base_vals * ramp_vals.reshape(1, ELEMS, 1)).astype(jnp.float32)


def plant(entries, stream_key, smallest, high):
    shape = entries.shape
    place = [jax.random.randint(jax.random.fold_in(stream_key, axis), (), 0, shape[axis]) for axis in range(len(shape))]
    entries = entries.at[tuple(place)].set(smallest)
    longest = shape.index(max(shape))
    place[longest] = (place[longest] + 1) % shape[longest]
    return entries.at[tuple(place)].set(high)


def shard_levels(stream_key, shape, split, least, largest):
    gain, own = 1.0, jax.random.fold_in(stream_key, 6)
    for axis_at, blocks in split:
        steps = jnp.exp(jax.random.uniform(jax.random.fold_in(own, axis_at), (blocks,), jnp.float32, least / len(split), largest / len(split)))
        gain = gain * jnp.repeat(steps, shape[axis_at] // blocks).reshape([-1 if axis == axis_at else 1 for axis in range(len(shape))])
    return gain


def gaussian(stream_key, dims, spread, bound, cuts=(), held_as=jnp.bfloat16):
    factor_of = shard_levels(stream_key, dims, cuts, -0.22, 0.18) if cuts else 1.0
    values = jax.random.normal(stream_key, dims, jnp.float32) * spread * factor_of
    return jnp.minimum(jnp.maximum(values, -bound), bound).astype(held_as)


def setup_inputs(seed: int = 0) -> dict:
    arg_keys = jax.random.split(jax.random.key(seed), 5)
    return {
        "old_basis": gaussian(arg_keys[0], (KB, ELEMS, PTS), 1.0, 6.0, ((1, 32),), jnp.float32),
        "restart_coeffs": gaussian(arg_keys[1], (KB,), 0.25, 1.0, (), jnp.float32),
        "geometry": draw_geometry(jax.random.fold_in(arg_keys[4], 71), 0),
        "orientation": plant(jax.random.randint(arg_keys[3], (6, ELEMS), 0, 8), jax.random.fold_in(arg_keys[3], 1), 0, 7).astype(jnp.int32),
    }


highest = lax.Precision.HIGHEST
epsilon = 1e-06

def legendre_columns(nodes, degree):
    columns = [nodes * 0.0 + 1.0, nodes * 1.0]
    for order in range(2, degree + 1):
        columns.append(((2 * order - 1) * nodes * columns[order - 1] - (order - 1) * columns[order - 2]) / order)
    return columns

def gll_derivative(extent):
    degree = extent - 1
    nodes = np.cos(np.pi * np.arange(extent) / degree)
    for sweep in range(100):
        columns = legendre_columns(nodes, degree)
        nodes = nodes - (nodes * columns[degree] - columns[degree - 1]) / (extent * columns[degree])
    gll_nodes = nodes[::-1] * 1.0
    values = legendre_columns(gll_nodes, degree)[degree]
    matrix = np.zeros((extent, extent))
    for row_idx in range(extent):
        for col_idx in range(extent):
            if row_idx != col_idx:
                matrix[row_idx, col_idx] = values[row_idx] / (values[col_idx] * (gll_nodes[row_idx] - gll_nodes[col_idx]))
    matrix[0, 0] = -degree * (degree + 1) / 4.0
    matrix[extent - 1, extent - 1] = degree * (degree + 1) / 4.0
    return matrix

def face_point(face_kind, row_pos, col_pos, extent):
    far_end = extent - 1
    if face_kind == 0:
        return (0, row_pos, col_pos)
    if face_kind == 1:
        return (far_end, row_pos, col_pos)
    if face_kind == 2:
        return (row_pos, 0, col_pos)
    if face_kind == 3:
        return (row_pos, far_end, col_pos)
    if face_kind == 4:
        return (row_pos, col_pos, 0)
    return (row_pos, col_pos, far_end)

def spectral_tables(extent):
    matrix = gll_derivative(extent)
    identity = np.eye(extent)
    along_x = np.kron(np.kron(matrix, identity), identity)
    along_y = np.kron(np.kron(identity, matrix), identity)
    along_z = np.kron(np.kron(identity, identity), matrix)
    forward = np.concatenate([along_x.T, along_y.T, along_z.T], axis=1)
    backward = np.concatenate([along_x, along_y, along_z], axis=0)
    square = extent * extent
    select = np.zeros((extent ** 3, 6 * square))
    rotations = np.zeros((square, 8 * square))
    for face_kind in range(6):
        for row_pos in range(extent):
            for col_pos in range(extent):
                triple = face_point(face_kind, row_pos, col_pos, extent)
                point_idx = (triple[0] * extent + triple[1]) * extent + triple[2]
                select[point_idx, face_kind * square + row_pos * extent + col_pos] = 1.0
    for code_value in range(8):
        for row_pos in range(extent):
            for col_pos in range(extent):
                row_src = extent - 1 - row_pos if code_value % 2 == 1 else row_pos
                col_src = extent - 1 - col_pos if code_value // 2 % 2 == 1 else col_pos
                if code_value >= 4:
                    source = col_src * extent + row_src
                else:
                    source = row_src * extent + col_src
                rotations[source, code_value * square + row_pos * extent + col_pos] = 1.0
    return (jnp.asarray(forward, dtype=jnp.float32), jnp.asarray(backward, dtype=jnp.float32), jnp.asarray(select, dtype=jnp.float32), jnp.asarray(rotations, dtype=jnp.float32))

def stiffness(field_in, geom_cat, mass_term, forward, backward):
    gradients = jnp.dot(field_in, forward, precision=highest, preferred_element_type=jnp.float32)
    return jnp.dot(gradients * geom_cat, backward, precision=highest, preferred_element_type=jnp.float32) + mass_term * field_in

def local_faces(local_out, select):
    face_vals = jnp.dot(local_out, select, precision=highest, preferred_element_type=jnp.float32)
    return face_vals.reshape(face_vals.shape[:-1] + (6, face_vals.shape[-1] // 6))

def shift_lower(values, direction):
    extent = values.shape[direction]
    leading = jnp.zeros_like(lax.slice_in_dim(values, 0, 1, axis=direction))
    return jnp.concatenate([leading, lax.slice_in_dim(values, 0, extent - 1, axis=direction)], axis=direction)

def shift_upper(values, direction):
    extent = values.shape[direction]
    trailing = jnp.zeros_like(lax.slice_in_dim(values, 0, 1, axis=direction))
    return jnp.concatenate([lax.slice_in_dim(values, 1, extent, axis=direction), trailing], axis=direction)

def assemble(local_out, incoming, orient_block, select, rotations):
    rotated = jnp.dot(incoming, rotations, precision=highest, preferred_element_type=jnp.float32)
    rotated = rotated.reshape(incoming.shape[:-1] + (8, incoming.shape[-1]))
    chosen_mask = orient_block[..., None] == jnp.arange(8, dtype=jnp.int32)
    chosen = lax.optimization_barrier(jnp.sum(jnp.where(chosen_mask[..., None], rotated, 0.0), axis=-2))
    flattened = chosen.reshape(chosen.shape[:-2] + (chosen.shape[-2] * chosen.shape[-1],))
    return local_out + jnp.dot(flattened, select.T, precision=highest, preferred_element_type=jnp.float32)

def to_grid(values):
    last_dim = values.shape[-1]
    shaped = values.reshape(N_WIDE, N_NARROW, EX, EY, EZ, last_dim).transpose(2, 1, 3, 0, 4, 5)
    return shaped.reshape(EX, N_NARROW * EY, N_WIDE * EZ, last_dim)

def from_grid(values):
    last_dim = values.shape[-1]
    shaped = values.reshape(EX, N_NARROW, EY, N_WIDE, EZ, last_dim).transpose(3, 1, 0, 2, 4, 5)
    return shaped.reshape(-1, last_dim)

def reference(old_basis, restart_coeffs, geometry, orientation):
    forward, backward, select, rotations = spectral_tables(NP)
    kept = old_basis.shape[0]
    total = float(old_basis.shape[1] * old_basis.shape[2])
    geom_cat = to_grid(jnp.concatenate([geometry[0], geometry[1], geometry[2]], axis=-1))
    mass_term = to_grid(geometry[3])
    orient_block = to_grid(orientation.T)
    flat_basis = old_basis.reshape(kept, -1)

    def operate(vector):
        local_out = stiffness(to_grid(vector), geom_cat, mass_term, forward, backward)
        face_vals = local_faces(local_out, select)
        incoming = jnp.stack([shift_lower(face_vals[..., 1, :], 0), shift_upper(face_vals[..., 0, :], 0), shift_lower(face_vals[..., 3, :], 1), shift_upper(face_vals[..., 2, :], 1), shift_lower(face_vals[..., 5, :], 2), shift_upper(face_vals[..., 4, :], 2)], axis=-2)
        return from_grid(assemble(local_out, incoming, orient_block, select, rotations))

    def inner(vector):
        return jnp.dot(flat_basis, vector.reshape(-1), precision=highest, preferred_element_type=jnp.float32) / total

    def combine(weights):
        return jnp.einsum('k,kep->ep', weights, old_basis, precision=highest, preferred_element_type=jnp.float32)
    start_vec = combine(restart_coeffs)
    image_one = operate(start_vec)
    first_proj = inner(image_one)
    residue_one = image_one - combine(first_proj)
    first_norm = jnp.sqrt(jnp.sum(residue_one * residue_one) / total + epsilon)
    first_vec = residue_one / first_norm
    image_two = operate(first_vec)
    second_proj = inner(image_two)
    second_self = jnp.sum(first_vec * image_two) / total
    residue_two = image_two - combine(second_proj) - second_self * first_vec
    second_norm = jnp.sqrt(jnp.sum(residue_two * residue_two) / total + epsilon)
    second_vec = residue_two / second_norm
    new_basis = jnp.stack([first_vec, second_vec])
    row_first = jnp.concatenate([first_proj, jnp.stack([first_norm, jnp.zeros_like(first_norm)])])
    row_second = jnp.concatenate([second_proj, jnp.stack([second_self, second_norm])])
    return (new_basis, jnp.stack([row_first, row_second]))
```

```python
import functools

import jax
import jax.numpy as jnp
import numpy as np
from jax import lax
from jax.experimental import pallas as pl
from jax.experimental.pallas import tpu as pltpu
from jax.sharding import PartitionSpec as P

NP = 8
EX = 4
EY = 4
EZ = 4
LANES = 128
FACE = NP * NP
MESH = pl.DeviceIdType.MESH
highest = lax.Precision.HIGHEST
epsilon = 1e-06


def legendre_columns(nodes, degree):
    columns = [nodes * 0.0 + 1.0, nodes * 1.0]
    for order in range(2, degree + 1):
        columns.append(
            ((2 * order - 1) * nodes * columns[order - 1] - (order - 1) * columns[order - 2])
            / order
        )
    return columns


def gll_derivative(extent):
    degree = extent - 1
    nodes = np.cos(np.pi * np.arange(extent) / degree)
    for sweep in range(100):
        columns = legendre_columns(nodes, degree)
        nodes = nodes - (nodes * columns[degree] - columns[degree - 1]) / (extent * columns[degree])
    gll_nodes = nodes[::-1] * 1.0
    values = legendre_columns(gll_nodes, degree)[degree]
    matrix = np.zeros((extent, extent))
    for row_idx in range(extent):
        for col_idx in range(extent):
            if row_idx != col_idx:
                matrix[row_idx, col_idx] = values[row_idx] / (
                    values[col_idx] * (gll_nodes[row_idx] - gll_nodes[col_idx])
                )
    matrix[0, 0] = -degree * (degree + 1) / 4.0
    matrix[extent - 1, extent - 1] = degree * (degree + 1) / 4.0
    return matrix


def tables():
    matrix = gll_derivative(NP)
    identity = np.eye(NP)
    pair = np.eye(2)
    along_y = np.kron(pair, np.kron(matrix, identity))
    along_z = np.kron(pair, np.kron(identity, matrix))
    forward = np.concatenate([along_y.T, along_z.T], axis=1)
    backward = np.concatenate([along_y, along_z], axis=0)
    tiles = NP // 2
    coef = np.zeros((2, tiles, tiles, 2, LANES))
    for way, table in enumerate((matrix, matrix.T)):
        for out_tile in range(tiles):
            for in_tile in range(tiles):
                for half in range(2):
                    lanes = slice(half * FACE, (half + 1) * FACE)
                    row = 2 * out_tile + half
                    coef[way, out_tile, in_tile, 0, lanes] = table[row, 2 * in_tile + half]
                    coef[way, out_tile, in_tile, 1, lanes] = table[row, 2 * in_tile + 1 - half]
    return (
        jnp.asarray(forward, jnp.float32),
        jnp.asarray(backward, jnp.float32),
        jnp.asarray(coef.reshape(-1, LANES), jnp.float32),
    )


def take_lanes(values, index):
    return jnp.take_along_axis(values, index, axis=1, mode="promise_in_bounds")


def rotated(row, col, code):
    row = row ^ (7 * (code & 1))
    col = col ^ (7 * ((code >> 1) & 1))
    return jnp.where((code & 4) != 0, col * NP + row, row * NP + col)


def kernel(
    n_wide,
    n_narrow,
    coeffs,
    basis_hbm,
    geom_hbm,
    orient,
    forward_hbm,
    backward_hbm,
    coef_hbm,
    out,
    hess,
    basis,
    geom,
    forward,
    backward,
    coef,
    index,
    orient_pad,
    image,
    first,
    face_y,
    face_z,
    halo_y,
    halo_z,
    outbox,
    inbox,
    row_out,
    row_in,
    load_sem,
    halo_send,
    halo_recv,
    row_send,
    row_recv,
):
    wide = lax.axis_index("wide")
    narrow = lax.axis_index("narrow")
    devices = n_wide * n_narrow
    me = wide * n_narrow + narrow
    kept, elements, points = basis.shape
    tiles = points // LANES
    total = float(elements * points * devices)

    def load(source, target, slot):
        return pltpu.make_async_copy(source, target, load_sem.at[slot])

    chunk = kept // 4
    loads = [
        load(basis_hbm.at[pl.ds(part * chunk, chunk)], basis.at[pl.ds(part * chunk, chunk)], part)
        for part in range(4)
    ]
    loads += [
        load(forward_hbm, forward, 4),
        load(geom_hbm, geom, 5),
        load(backward_hbm, backward, 6),
        load(coef_hbm, coef, 7),
    ]
    for copy in loads:
        copy.start()

    inbox[...] = jnp.zeros_like(inbox)

    def peer(step):
        other = lax.rem(me + step, devices)
        return (other // n_narrow, lax.rem(other, n_narrow))

    barrier = pltpu.get_barrier_semaphore()

    def greet(step, carry):
        pl.semaphore_signal(barrier, inc=1, device_id=peer(step), device_id_type=MESH)
        return carry

    lax.fori_loop(1, devices, greet, 0)

    lane = lax.broadcasted_iota(jnp.int32, (elements, LANES), 1)
    line = lax.broadcasted_iota(jnp.int32, (elements, LANES), 0)
    low_half = lane < FACE
    half = lane // FACE
    mid = (lane // NP) % NP
    fast = lane % NP
    row_y = (line // EZ) % EY
    row_z = line % EZ
    at_y = (mid == 0) | (mid == NP - 1)
    at_z = (fast == 0) | (fast == NP - 1)

    orient_pad[...] = jnp.zeros_like(orient_pad)
    orient_pad[pl.ds(0, 6), pl.ds(0, elements)] = orient[...]
    codes = jnp.transpose(orient_pad[...])[:elements]
    code = [jnp.broadcast_to(codes[:, f : f + 1], (elements, LANES)) for f in range(6)]
    code_x = jnp.where(low_half, code[0], code[1])
    index[2 * tiles] = rotated(mid, fast, code_x) + jnp.where(low_half, FACE, 0)
    code_y = jnp.where(mid == 0, code[2], code[3])
    code_z = jnp.where(fast == 0, code[4], code[5])
    for tile in range(tiles):
        first_pos = 2 * tile + half
        index[tile] = rotated(first_pos, fast, code_y) + jnp.where(mid == 0, FACE, 0)
        index[tiles + tile] = rotated(first_pos, mid, code_z) + jnp.where(fast == 0, FACE, 0)

    pick_y = (mid % 2) * FACE + half * (FACE - NP) + fast
    pick_z = (mid % 2) * FACE + fast * NP + half * (NP - 1)
    source_tile = mid // 2

    def tile_of(values, tile):
        return values[:, tile * LANES : (tile + 1) * LANES]

    def swap(values):
        return pltpu.roll(values, FACE, axis=1)

    def along_x(parts, way):
        swapped = [swap(part) for part in parts]
        outs = []
        for out_tile in range(tiles):
            acc = None
            for in_tile in range(tiles):
                at = ((way * tiles + out_tile) * tiles + in_tile) * 2
                term = (
                    coef[pl.ds(at, 1), :] * parts[in_tile]
                    + coef[pl.ds(at + 1, 1), :] * swapped[in_tile]
                )
                acc = term if acc is None else acc + term
            outs.append(acc)
        return outs

    def local(parts):
        stacked = jnp.concatenate(parts, axis=0)
        grads = jnp.dot(
            stacked, forward[...], precision=highest, preferred_element_type=jnp.float32
        )
        geom_y = jnp.concatenate([geom[1, :, pl.ds(t * LANES, LANES)] for t in range(tiles)], axis=0)
        geom_z = jnp.concatenate([geom[2, :, pl.ds(t * LANES, LANES)] for t in range(tiles)], axis=0)
        flux = jnp.concatenate([grads[:, :LANES] * geom_y, grads[:, LANES:] * geom_z], axis=1)
        back = jnp.dot(
            flux, backward[...], precision=highest, preferred_element_type=jnp.float32
        )
        grad_x = along_x(parts, 0)
        flux_x = [grad_x[t] * geom[0, :, pl.ds(t * LANES, LANES)] for t in range(tiles)]
        back_x = along_x(flux_x, 1)
        return [
            back[t * elements : (t + 1) * elements]
            + back_x[t]
            + geom[3, :, pl.ds(t * LANES, LANES)] * parts[t]
            for t in range(tiles)
        ]

    def faces(parts, pick):
        found = take_lanes(parts[0], pick)
        for tile in range(1, tiles):
            found = jnp.where(source_tile == tile, take_lanes(parts[tile], pick), found)
        return found

    has = (narrow > 0, narrow < n_narrow - 1, wide > 0, wide < n_wide - 1)
    where_to = ((wide, narrow - 1), (wide, narrow + 1), (wide - 1, narrow), (wide + 1, narrow))

    def face_copy(step, side):
        return pltpu.make_async_remote_copy(
            src_ref=outbox.at[step, side],
            dst_ref=inbox.at[step, side ^ 1],
            send_sem=halo_send.at[step, side],
            recv_sem=halo_recv.at[step, side ^ 1],
            device_id=where_to[side],
            device_id_type=MESH,
        )

    def face_arrival(step, side):
        return pltpu.make_async_copy(
            inbox.at[step, side], inbox.at[step, side], halo_recv.at[step, side]
        )

    def operate(parts, step, ready):
        result = local(parts)
        found_y = faces(result, pick_y)
        found_z = faces(result, pick_z)
        face_y[...] = found_y
        face_z[...] = found_z
        for ex in range(EX):
            outbox[step, 0, pl.ds(ex * EZ, EZ), :] = face_y[pl.ds(ex * EY * EZ, EZ), :]
            outbox[step, 1, pl.ds(ex * EZ, EZ), :] = face_y[pl.ds(ex * EY * EZ + (EY - 1) * EZ, EZ), :]
        outbox[step, 2] = face_z[pl.ds(0, EX * EY, stride=EZ), :]
        outbox[step, 3] = face_z[pl.ds(EZ - 1, EX * EY, stride=EZ), :]
        ready()
        for side in (2, 3, 0, 1):

            @pl.when(has[side])
            def _():
                face_copy(step, side).start()

        face_x = jnp.where(low_half, result[0], result[tiles - 1])
        width = EY * EZ
        blank = jnp.zeros((width, LANES), jnp.float32)
        in_x = jnp.where(
            low_half,
            jnp.concatenate([face_x[width:], blank], axis=0),
            jnp.concatenate([blank, face_x[: elements - width]], axis=0),
        )
        in_y = jnp.where(
            low_half, pltpu.roll(found_y, elements - EZ, axis=0), pltpu.roll(found_y, EZ, axis=0)
        )
        in_z = jnp.where(
            low_half, pltpu.roll(found_z, elements - 1, axis=0), pltpu.roll(found_z, 1, axis=0)
        )
        got_x = take_lanes(in_x, index[2 * tiles])
        result[0] = result[0] + jnp.where(low_half, got_x, 0.0)
        result[tiles - 1] = result[tiles - 1] + jnp.where(low_half, 0.0, got_x)

        for side in range(4):

            @pl.when(has[side])
            def _():
                face_arrival(step, side).wait()

        for ex in range(EX):
            halo_y[pl.ds(ex * EY * EZ, EZ), :] = inbox[step, 0, pl.ds(ex * EZ, EZ), :]
            halo_y[pl.ds(ex * EY * EZ + (EY - 1) * EZ, EZ), :] = inbox[step, 1, pl.ds(ex * EZ, EZ), :]
        halo_z[pl.ds(0, EX * EY, stride=EZ), :] = inbox[step, 2]
        halo_z[pl.ds(EZ - 1, EX * EY, stride=EZ), :] = inbox[step, 3]
        edge_y = row_y == jnp.where(low_half, EY - 1, 0)
        edge_z = row_z == jnp.where(low_half, EZ - 1, 0)
        in_y = jnp.where(edge_y, halo_y[...], in_y)
        in_z = jnp.where(edge_z, halo_z[...], in_z)
        return [
            result[t]
            + jnp.where(at_y, take_lanes(in_y, index[t]), 0.0)
            + jnp.where(at_z, take_lanes(in_z, index[tiles + t]), 0.0)
            for t in range(tiles)
        ]

    def folded(values):
        acc = tile_of(values, 0)
        for tile in range(1, tiles):
            acc = acc + tile_of(values, tile)
        return jnp.sum(acc.reshape(elements // 8, 8, LANES), axis=0)

    def to_row(partials):
        count = -(-len(partials) // 8) * 8
        rows = [jnp.sum(part, axis=0, keepdims=True) for part in partials]
        rows += [jnp.zeros((1, LANES), jnp.float32)] * (count - len(rows))
        block = jnp.concatenate(rows, axis=0)
        sums = jnp.sum(block, axis=1, keepdims=True)
        place = lax.broadcasted_iota(jnp.int32, (count, LANES), 0) == lax.broadcasted_iota(
            jnp.int32, (count, LANES), 1
        )
        return jnp.sum(jnp.where(place, sums, 0.0), axis=0, keepdims=True)

    def all_sum(row, phase):
        row_out[phase] = row
        row_in[phase, pl.ds(me, 1)] = row.reshape(1, 1, LANES)

        def send(step, carry):
            pltpu.make_async_remote_copy(
                src_ref=row_out.at[phase],
                dst_ref=row_in.at[phase, me],
                send_sem=row_send.at[phase],
                recv_sem=row_recv.at[phase],
                device_id=peer(step),
                device_id_type=MESH,
            ).start()
            return carry

        lax.fori_loop(1, devices, send, 0)
        span = row_in.at[phase, pl.ds(0, devices - 1)]
        pltpu.make_async_copy(span, span, row_recv.at[phase]).wait()
        return jnp.sum(row_in[phase], axis=0)

    def weight(row, at):
        return row[:, at : at + 1]

    start = None
    for part in range(4):
        loads[part].wait()
        for at in range(part * chunk, (part + 1) * chunk):
            term = coeffs[at] * basis[at]
            start = term if start is None else start + term
    for copy in loads[4:]:
        copy.wait()

    def greeted():
        pl.semaphore_wait(barrier, devices - 1)

    image_parts = operate([tile_of(start, t) for t in range(tiles)], 0, greeted)
    for t in range(tiles):
        image[:, pl.ds(t * LANES, LANES)] = image_parts[t]
    row = to_row([folded(basis[at] * image[...]) for at in range(kept)])
    proj_one = all_sum(row, 0) / total
    acc = image[...]
    for at in range(kept):
        acc = acc - weight(proj_one, at) * basis[at]
    first[...] = acc

    image_parts = operate(
        [first[:, pl.ds(t * LANES, LANES)] for t in range(tiles)], 1, lambda: None
    )
    for t in range(tiles):
        image[:, pl.ds(t * LANES, LANES)] = image_parts[t]
    row = to_row(
        [folded(basis[at] * image[...]) for at in range(kept)]
        + [folded(first[...] * first[...]), folded(first[...] * image[...])]
    )
    sums = all_sum(row, 1) / total
    norm_one = jnp.sqrt(weight(sums, kept) + epsilon)
    scale_one = 1.0 / norm_one
    proj_two = sums * scale_one
    self_two = weight(sums, kept + 1) * scale_one * scale_one
    acc = image[...] - (self_two * first[...])
    for at in range(kept):
        acc = acc - weight(sums, at) * basis[at]
    acc = acc * scale_one
    out[0] = first[...] * scale_one
    image[...] = acc
    square = all_sum(to_row([folded(acc * acc)]), 2) / total
    norm_two = jnp.sqrt(weight(square, 0) + epsilon)
    out[1] = image[...] * (1.0 / norm_two)

    spot = lax.broadcasted_iota(jnp.int32, (1, LANES), 1)
    row_first = jnp.where(spot < kept, proj_one, jnp.where(spot == kept, norm_one, 0.0))
    row_second = jnp.where(spot < kept, proj_two, jnp.where(spot == kept, self_two, norm_two))
    hess[pl.ds(0, 1), :] = row_first[:, : kept + 2]
    hess[pl.ds(1, 1), :] = row_second[:, : kept + 2]

    for step in range(2):
        for side in range(4):

            @pl.when(has[side])
            def _():
                face_copy(step, side).wait_send()

    for phase in range(3):
        span = row_in.at[phase, pl.ds(0, devices - 1)]
        pltpu.make_async_copy(span, span, row_send.at[phase]).wait()


def on_device(n_wide, n_narrow, old_basis, restart_coeffs, geometry, orientation):
    kept, elements, points = old_basis.shape
    tiles = points // LANES
    devices = n_wide * n_narrow
    forward, backward, coef = tables()
    anywhere = pl.BlockSpec(memory_space=pl.ANY)
    vmem = pl.BlockSpec(memory_space=pltpu.VMEM)
    f32 = jnp.float32
    border = EX * EY
    return pl.pallas_call(
        functools.partial(kernel, n_wide, n_narrow),
        out_shape=(
            jax.ShapeDtypeStruct((2, elements, points), f32),
            jax.ShapeDtypeStruct((2, kept + 2), f32),
        ),
        in_specs=[
            pl.BlockSpec(memory_space=pltpu.SMEM),
            anywhere,
            anywhere,
            vmem,
            anywhere,
            anywhere,
            anywhere,
        ],
        out_specs=(vmem, vmem),
        scratch_shapes=[
            pltpu.VMEM(old_basis.shape, f32),
            pltpu.VMEM(geometry.shape, f32),
            pltpu.VMEM(forward.shape, f32),
            pltpu.VMEM(backward.shape, f32),
            pltpu.VMEM(coef.shape, f32),
            pltpu.VMEM((2 * tiles + 1, elements, LANES), jnp.int32),
            pltpu.VMEM((8, LANES), jnp.int32),
            pltpu.VMEM((elements, points), f32),
            pltpu.VMEM((elements, points), f32),
            pltpu.VMEM((elements, LANES), f32),
            pltpu.VMEM((elements, LANES), f32),
            pltpu.VMEM((elements, LANES), f32),
            pltpu.VMEM((elements, LANES), f32),
            pltpu.VMEM((2, 4, border, LANES), f32),
            pltpu.VMEM((2, 4, border, LANES), f32),
            pltpu.VMEM((3, 1, LANES), f32),
            pltpu.VMEM((3, devices, 1, LANES), f32),
            pltpu.SemaphoreType.DMA((8,)),
            pltpu.SemaphoreType.DMA((2, 4)),
            pltpu.SemaphoreType.DMA((2, 4)),
            pltpu.SemaphoreType.DMA((3,)),
            pltpu.SemaphoreType.DMA((3,)),
        ],
        compiler_params=pltpu.CompilerParams(collective_id=0, has_side_effects=True),
        name="arnoldi",
    )(restart_coeffs, old_basis, geometry, orientation, forward, backward, coef)


def solution(mesh):
    in_specs = (
        P(None, ("wide", "narrow"), None),
        P(),
        P(None, ("wide", "narrow"), None),
        P(None, ("wide", "narrow")),
    )
    out_specs = (P(None, ("wide", "narrow"), None), P())
    return jax.shard_map(
        functools.partial(on_device, mesh.shape["wide"], mesh.shape["narrow"]),
        mesh=mesh,
        in_specs=in_specs,
        out_specs=out_specs,
        check_vma=False,
    )
```

```python
import functools

import jax
import jax.numpy as jnp
import numpy as np
from jax import lax
from jax.experimental import pallas as pl
from jax.experimental.pallas import tpu as pltpu
from jax.sharding import PartitionSpec as P

NP = 8
EX = 4
EY = 4
EZ = 4
LANES = 128
FACE = NP * NP
MESH = pl.DeviceIdType.MESH
highest = lax.Precision.HIGHEST
epsilon = 1e-06


def legendre_columns(nodes, degree):
    columns = [nodes * 0.0 + 1.0, nodes * 1.0]
    for order in range(2, degree + 1):
        columns.append(
            ((2 * order - 1) * nodes * columns[order - 1] - (order - 1) * columns[order - 2])
            / order
        )
    return columns


def gll_derivative(extent):
    degree = extent - 1
    nodes = np.cos(np.pi * np.arange(extent) / degree)
    for sweep in range(100):
        columns = legendre_columns(nodes, degree)
        nodes = nodes - (nodes * columns[degree] - columns[degree - 1]) / (extent * columns[degree])
    gll_nodes = nodes[::-1] * 1.0
    values = legendre_columns(gll_nodes, degree)[degree]
    matrix = np.zeros((extent, extent))
    for row_idx in range(extent):
        for col_idx in range(extent):
            if row_idx != col_idx:
                matrix[row_idx, col_idx] = values[row_idx] / (
                    values[col_idx] * (gll_nodes[row_idx] - gll_nodes[col_idx])
                )
    matrix[0, 0] = -degree * (degree + 1) / 4.0
    matrix[extent - 1, extent - 1] = degree * (degree + 1) / 4.0
    return matrix


def tables():
    matrix = gll_derivative(NP)
    identity = np.eye(NP)
    pair = np.eye(2)
    along_y = np.kron(pair, np.kron(matrix, identity))
    along_z = np.kron(pair, np.kron(identity, matrix))
    forward = np.concatenate([along_y.T, along_z.T], axis=1)
    backward = np.concatenate([along_y, along_z], axis=0)
    tiles = NP // 2
    coef = np.zeros((2, tiles, tiles, 2, LANES))
    for way, table in enumerate((matrix, matrix.T)):
        for out_tile in range(tiles):
            for in_tile in range(tiles):
                for half in range(2):
                    lanes = slice(half * FACE, (half + 1) * FACE)
                    row = 2 * out_tile + half
                    coef[way, out_tile, in_tile, 0, lanes] = table[row, 2 * in_tile + half]
                    coef[way, out_tile, in_tile, 1, lanes] = table[row, 2 * in_tile + 1 - half]
    return (
        jnp.asarray(forward, jnp.float32),
        jnp.asarray(backward, jnp.float32),
        jnp.asarray(coef.reshape(-1, LANES), jnp.float32),
    )


def pair_rows(kept):
    count = kept + 2
    listed = [(at, kept + 1) for at in range(count)]
    listed += [(at, kept) for at in range(kept + 1)]
    block = 4
    for left in range(0, kept, block):
        for right in range(left, kept, block):
            for one in range(left, left + block):
                for two in range(max(right, one), right + block):
                    listed.append((one, two))
    return -(-len(listed) // LANES), listed


def take_lanes(values, index):
    return jnp.take_along_axis(values, index, axis=1, mode="promise_in_bounds")


def rotated(row, col, code):
    row = row ^ (7 * (code & 1))
    col = col ^ (7 * ((code >> 1) & 1))
    return jnp.where((code & 4) != 0, col * NP + row, row * NP + col)


def kernel(
    n_wide,
    n_narrow,
    coeffs,
    basis_hbm,
    geom_hbm,
    orient,
    forward_hbm,
    backward_hbm,
    coef_hbm,
    pairs_hbm,
    out,
    hess,
    basis,
    geom,
    forward,
    backward,
    coef,
    index,
    orient_pad,
    image,
    first,
    face_y,
    face_z,
    halo_y,
    halo_z,
    outbox,
    inbox,
    pairs,
    row_out,
    row_in,
    pair_out,
    pair_in,
    load_sem,
    halo_send,
    halo_recv,
    row_send,
    row_recv,
):
    wide = lax.axis_index("wide")
    narrow = lax.axis_index("narrow")
    devices = n_wide * n_narrow
    me = wide * n_narrow + narrow
    kept, elements, points = basis.shape
    tiles = points // LANES
    total = float(elements * points * devices)

    def load(source, target, slot):
        return pltpu.make_async_copy(source, target, load_sem.at[slot])

    chunk = kept // 4
    loads = [
        load(basis_hbm.at[pl.ds(part * chunk, chunk)], basis.at[pl.ds(part * chunk, chunk)], part)
        for part in range(4)
    ]
    loads += [
        load(forward_hbm, forward, 4),
        load(geom_hbm, geom, 5),
        load(backward_hbm, backward, 6),
        load(coef_hbm, coef, 7),
        load(pairs_hbm, pairs, 8),
    ]
    for copy in loads:
        copy.start()

    messages = ((row_out, row_in), (pair_out, pair_in))
    inbox[...] = jnp.zeros_like(inbox)

    def peer(step):
        if devices & (devices - 1):
            other = lax.rem(me + step, devices)
        else:
            other = me
            for bit in range(devices.bit_length() - 1):
                if step >> bit & 1:
                    other = other + (1 - 2 * lax.rem(me // 2**bit, 2)) * 2**bit
        return (other // n_narrow, lax.rem(other, n_narrow))

    def each_peer(act):
        if devices <= 64:
            for step in range(devices - 1, 0, -1):
                act(peer(step))
        else:

            def body(step, carry):
                other = lax.rem(me + step, devices)
                act((other // n_narrow, lax.rem(other, n_narrow)))
                return carry

            lax.fori_loop(1, devices, body, 0)

    barrier = pltpu.get_barrier_semaphore()

    def greet(where):
        pl.semaphore_signal(barrier, inc=1, device_id=where, device_id_type=MESH)

    each_peer(greet)

    lane = lax.broadcasted_iota(jnp.int32, (elements, LANES), 1)
    line = lax.broadcasted_iota(jnp.int32, (elements, LANES), 0)
    low_half = lane < FACE
    half = lane // FACE
    mid = (lane // NP) % NP
    fast = lane % NP
    row_y = (line // EZ) % EY
    row_z = line % EZ
    at_y = (mid == 0) | (mid == NP - 1)
    at_z = (fast == 0) | (fast == NP - 1)

    orient_pad[...] = jnp.zeros_like(orient_pad)
    orient_pad[pl.ds(0, 6), pl.ds(0, elements)] = orient[...]
    codes = jnp.transpose(orient_pad[...])[:elements]
    code = [jnp.broadcast_to(codes[:, f : f + 1], (elements, LANES)) for f in range(6)]
    code_x = jnp.where(low_half, code[0], code[1])
    index[2 * tiles] = rotated(mid, fast, code_x) + jnp.where(low_half, FACE, 0)
    code_y = jnp.where(mid == 0, code[2], code[3])
    code_z = jnp.where(fast == 0, code[4], code[5])
    for tile in range(tiles):
        first_pos = 2 * tile + half
        index[tile] = rotated(first_pos, fast, code_y) + jnp.where(mid == 0, FACE, 0)
        index[tiles + tile] = rotated(first_pos, mid, code_z) + jnp.where(fast == 0, FACE, 0)

    pick_y = (mid % 2) * FACE + half * (FACE - NP) + fast
    pick_z = (mid % 2) * FACE + fast * NP + half * (NP - 1)
    source_tile = mid // 2

    def tile_of(values, tile):
        return values[:, tile * LANES : (tile + 1) * LANES]

    def swap(values):
        return pltpu.roll(values, FACE, axis=1)

    def along_x(parts, way):
        swapped = [swap(part) for part in parts]
        outs = []
        for out_tile in range(tiles):
            acc = None
            for in_tile in range(tiles):
                at = ((way * tiles + out_tile) * tiles + in_tile) * 2
                term = (
                    coef[pl.ds(at, 1), :] * parts[in_tile]
                    + coef[pl.ds(at + 1, 1), :] * swapped[in_tile]
                )
                acc = term if acc is None else acc + term
            outs.append(acc)
        return outs

    def local(parts):
        stacked = jnp.concatenate(parts, axis=0)
        grads = jnp.dot(
            stacked, forward[...], precision=highest, preferred_element_type=jnp.float32
        )
        geom_y = jnp.concatenate([geom[1, :, pl.ds(t * LANES, LANES)] for t in range(tiles)], axis=0)
        geom_z = jnp.concatenate([geom[2, :, pl.ds(t * LANES, LANES)] for t in range(tiles)], axis=0)
        flux = jnp.concatenate([grads[:, :LANES] * geom_y, grads[:, LANES:] * geom_z], axis=1)
        back = jnp.dot(
            flux, backward[...], precision=highest, preferred_element_type=jnp.float32
        )
        grad_x = along_x(parts, 0)
        flux_x = [grad_x[t] * geom[0, :, pl.ds(t * LANES, LANES)] for t in range(tiles)]
        back_x = along_x(flux_x, 1)
        return [
            back[t * elements : (t + 1) * elements]
            + back_x[t]
            + geom[3, :, pl.ds(t * LANES, LANES)] * parts[t]
            for t in range(tiles)
        ]

    def faces(parts, pick):
        found = take_lanes(parts[0], pick)
        for tile in range(1, tiles):
            found = jnp.where(source_tile == tile, take_lanes(parts[tile], pick), found)
        return found

    has = (narrow > 0, narrow < n_narrow - 1, wide > 0, wide < n_wide - 1)
    where_to = ((wide, narrow - 1), (wide, narrow + 1), (wide - 1, narrow), (wide + 1, narrow))

    def face_copy(step, side):
        return pltpu.make_async_remote_copy(
            src_ref=outbox.at[step, side],
            dst_ref=inbox.at[step, side ^ 1],
            send_sem=halo_send.at[step, side],
            recv_sem=halo_recv.at[step, side ^ 1],
            device_id=where_to[side],
            device_id_type=MESH,
        )

    def face_arrival(step, side):
        return pltpu.make_async_copy(
            inbox.at[step, side], inbox.at[step, side], halo_recv.at[step, side]
        )

    def operate(parts, step, ready, beside=lambda: None):
        result = local(parts)
        found_y = faces(result, pick_y)
        found_z = faces(result, pick_z)
        face_y[...] = found_y
        face_z[...] = found_z
        for ex in range(EX):
            outbox[step, 0, pl.ds(ex * EZ, EZ), :] = face_y[pl.ds(ex * EY * EZ, EZ), :]
            outbox[step, 1, pl.ds(ex * EZ, EZ), :] = face_y[pl.ds(ex * EY * EZ + (EY - 1) * EZ, EZ), :]
        outbox[step, 2] = face_z[pl.ds(0, EX * EY, stride=EZ), :]
        outbox[step, 3] = face_z[pl.ds(EZ - 1, EX * EY, stride=EZ), :]
        ready()
        for side in (2, 3, 0, 1):

            @pl.when(has[side])
            def _():
                face_copy(step, side).start()

        face_x = jnp.where(low_half, result[0], result[tiles - 1])
        width = EY * EZ
        blank = jnp.zeros((width, LANES), jnp.float32)
        in_x = jnp.where(
            low_half,
            jnp.concatenate([face_x[width:], blank], axis=0),
            jnp.concatenate([blank, face_x[: elements - width]], axis=0),
        )
        in_y = jnp.where(
            low_half, pltpu.roll(found_y, elements - EZ, axis=0), pltpu.roll(found_y, EZ, axis=0)
        )
        in_z = jnp.where(
            low_half, pltpu.roll(found_z, elements - 1, axis=0), pltpu.roll(found_z, 1, axis=0)
        )
        got_x = take_lanes(in_x, index[2 * tiles])
        result[0] = result[0] + jnp.where(low_half, got_x, 0.0)
        result[tiles - 1] = result[tiles - 1] + jnp.where(low_half, 0.0, got_x)

        beside()

        for side in range(4):

            @pl.when(has[side])
            def _():
                face_arrival(step, side).wait()

        for ex in range(EX):
            halo_y[pl.ds(ex * EY * EZ, EZ), :] = inbox[step, 0, pl.ds(ex * EZ, EZ), :]
            halo_y[pl.ds(ex * EY * EZ + (EY - 1) * EZ, EZ), :] = inbox[step, 1, pl.ds(ex * EZ, EZ), :]
        halo_z[pl.ds(0, EX * EY, stride=EZ), :] = inbox[step, 2]
        halo_z[pl.ds(EZ - 1, EX * EY, stride=EZ), :] = inbox[step, 3]
        edge_y = row_y == jnp.where(low_half, EY - 1, 0)
        edge_z = row_z == jnp.where(low_half, EZ - 1, 0)
        in_y = jnp.where(edge_y, halo_y[...], in_y)
        in_z = jnp.where(edge_z, halo_z[...], in_z)
        return [
            result[t]
            + jnp.where(at_y, take_lanes(in_y, index[t]), 0.0)
            + jnp.where(at_z, take_lanes(in_z, index[tiles + t]), 0.0)
            for t in range(tiles)
        ]

    def folded(values):
        acc = tile_of(values, 0)
        for tile in range(1, tiles):
            acc = acc + tile_of(values, tile)
        return jnp.sum(acc.reshape(elements // 8, 8, LANES), axis=0)

    def to_row(partials, begin=0):
        count = -(-len(partials) // 8) * 8
        rows = [jnp.sum(part, axis=0, keepdims=True) for part in partials]
        rows += [jnp.zeros((1, LANES), jnp.float32)] * (count - len(rows))
        block = jnp.concatenate(rows, axis=0)
        sums = jnp.sum(block, axis=1, keepdims=True)
        place = lax.broadcasted_iota(jnp.int32, (count, LANES), 0) + begin == lax.broadcasted_iota(
            jnp.int32, (count, LANES), 1
        )
        return jnp.sum(jnp.where(place, sums, 0.0), axis=0, keepdims=True)

    def all_sum(block, phase, beside):
        outgoing, incoming = messages[phase]
        outgoing[...] = block
        incoming[pl.ds(me, 1)] = block.reshape((1,) + block.shape)

        def send(where):
            pltpu.make_async_remote_copy(
                src_ref=outgoing,
                dst_ref=incoming.at[me],
                send_sem=row_send.at[phase],
                recv_sem=row_recv.at[phase],
                device_id=where,
                device_id_type=MESH,
            ).start()

        each_peer(send)
        result = beside()
        span = incoming.at[pl.ds(0, devices - 1)]
        pltpu.make_async_copy(span, span, row_recv.at[phase]).wait()
        return jnp.sum(incoming[...], axis=0), result

    def weight(row, at):
        return row[:, at : at + 1]

    start = None
    for part in range(4):
        loads[part].wait()
        for at in range(part * chunk, (part + 1) * chunk):
            term = coeffs[at] * basis[at]
            start = term if start is None else start + term
    for copy in loads[4:]:
        copy.wait()

    def greeted():
        pl.semaphore_wait(barrier, devices - 1)

    image_parts = operate([tile_of(start, t) for t in range(tiles)], 0, greeted)
    for t in range(tiles):
        image[:, pl.ds(t * LANES, LANES)] = image_parts[t]
    rows, listed = pair_rows(kept)
    fresh = 2 * kept + 3

    def gram():
        partials = []
        block = 4
        for left in range(0, kept, block):
            for right in range(left, kept, block):
                wanted = [
                    (one, two)
                    for one in range(left, left + block)
                    for two in range(max(right, one), right + block)
                ]

                def body(step, carry):
                    base = pl.multiple_of(step * 8, 8)
                    carry = list(carry)
                    for tile in range(tiles):
                        at = (pl.ds(base, 8), pl.ds(tile * LANES, LANES))
                        ones = [basis[(left + m,) + at] for m in range(block)]
                        twos = ones if left == right else [
                            basis[(right + m,) + at] for m in range(block)
                        ]
                        for spot, (one, two) in enumerate(wanted):
                            carry[spot] = carry[spot] + ones[one - left] * twos[two - right]
                    return tuple(carry)

                zero = jnp.zeros((8, LANES), jnp.float32)
                partials += list(
                    lax.fori_loop(0, elements // 8, body, (zero,) * len(wanted))
                )
        gram_rows = []
        for begin in range(0, rows * LANES, LANES):
            lo = max(begin, fresh)
            here = partials[lo - fresh : begin + LANES - fresh]
            row = to_row(here, lo - begin) if here else jnp.zeros((1, LANES), jnp.float32)
            gram_rows.append(row)
        return gram_rows

    row = to_row([folded(basis[at] * image[...]) for at in range(kept)])
    sums, gram_part = all_sum(row, 0, gram)
    proj_one = sums / total
    acc = image[...]
    for at in range(kept):
        acc = acc - weight(proj_one, at) * basis[at]
    first[...] = acc

    with_first = []

    def project_first():
        with_first.extend(
            [folded(basis[at] * first[...]) for at in range(kept)]
            + [folded(first[...] * first[...])]
        )

    image_parts = operate(
        [first[:, pl.ds(t * LANES, LANES)] for t in range(tiles)], 1, lambda: None, project_first
    )
    for t in range(tiles):
        image[:, pl.ds(t * LANES, LANES)] = image_parts[t]
    row = to_row(
        [folded(basis[at] * image[...]) for at in range(kept)]
        + [folded(first[...] * image[...]), folded(image[...] * image[...])]
        + with_first
    )
    block = jnp.concatenate([gram_part[0] + row] + gram_part[1:], axis=0)
    sums, _ = all_sum(block, 1, lambda: None)
    sums = sums / total
    along = sums[0:1]
    norm_one = jnp.sqrt(weight(along, fresh - 1) + epsilon)
    scale_one = 1.0 / norm_one
    proj_two = along * scale_one
    self_two = weight(along, kept) * scale_one * scale_one

    spot = lax.broadcasted_iota(jnp.int32, (8, LANES), 1)
    factor = jnp.broadcast_to(along, (8, LANES))
    factor = jnp.where(spot < kept, -factor, 0.0)
    factor = jnp.where(spot == kept, -self_two, factor)
    factor = jnp.where(spot == kept + 1, 1.0, factor)
    square = jnp.zeros((1, LANES), jnp.float32)
    for at in range(rows):
        left = jnp.broadcast_to(pairs[pl.ds(at, 1), :], (8, LANES))
        right = jnp.broadcast_to(pairs[pl.ds(rows + at, 1), :], (8, LANES))
        product = take_lanes(factor, left) * take_lanes(factor, right)
        product = jnp.where(left == right, product, 2.0 * product)
        used = spot + at * LANES < len(listed)
        square = square + jnp.where(used, product * sums[at : at + 1], 0.0)[0:1]
    square = jnp.maximum(jnp.sum(square, axis=1, keepdims=True), 0.0) * (scale_one * scale_one)
    norm_two = jnp.sqrt(square + epsilon)

    acc = image[...] - (self_two * first[...])
    for at in range(kept):
        acc = acc - weight(along, at) * basis[at]
    out[0] = first[...] * scale_one
    out[1] = acc * (scale_one / norm_two)

    spot = lax.broadcasted_iota(jnp.int32, (1, LANES), 1)
    row_first = jnp.where(spot < kept, proj_one, jnp.where(spot == kept, norm_one, 0.0))
    row_second = jnp.where(spot < kept, proj_two, jnp.where(spot == kept, self_two, norm_two))
    hess[pl.ds(0, 1), :] = row_first[:, : kept + 2]
    hess[pl.ds(1, 1), :] = row_second[:, : kept + 2]

    for step in range(2):
        for side in range(4):

            @pl.when(has[side])
            def _():
                face_copy(step, side).wait_send()

    for phase in range(2):
        span = messages[phase][1].at[pl.ds(0, devices - 1)]
        pltpu.make_async_copy(span, span, row_send.at[phase]).wait()


def on_device(n_wide, n_narrow, old_basis, restart_coeffs, geometry, orientation):
    kept, elements, points = old_basis.shape
    tiles = points // LANES
    devices = n_wide * n_narrow
    forward, backward, coef = tables()
    rows, listed = pair_rows(kept)
    pairs = np.zeros((2 * rows, LANES), np.int32)
    for at, (left, right) in enumerate(listed):
        pairs[at // LANES, at % LANES] = left
        pairs[rows + at // LANES, at % LANES] = right
    pairs = jnp.asarray(pairs)
    anywhere = pl.BlockSpec(memory_space=pl.ANY)
    vmem = pl.BlockSpec(memory_space=pltpu.VMEM)
    f32 = jnp.float32
    border = EX * EY
    shapes = ((2, elements, points), (2, kept + 2))
    held = pl.pallas_call(
        functools.partial(kernel, n_wide, n_narrow),
        out_shape=tuple(pltpu.VMEM(shape, f32) for shape in shapes),
        in_specs=[
            pl.BlockSpec(memory_space=pltpu.SMEM),
            anywhere,
            anywhere,
            vmem,
            anywhere,
            anywhere,
            anywhere,
            anywhere,
        ],
        out_specs=(vmem, vmem),
        scratch_shapes=[
            pltpu.VMEM(old_basis.shape, f32),
            pltpu.VMEM(geometry.shape, f32),
            pltpu.VMEM(forward.shape, f32),
            pltpu.VMEM(backward.shape, f32),
            pltpu.VMEM(coef.shape, f32),
            pltpu.VMEM((2 * tiles + 1, elements, LANES), jnp.int32),
            pltpu.VMEM((8, LANES), jnp.int32),
            pltpu.VMEM((elements, points), f32),
            pltpu.VMEM((elements, points), f32),
            pltpu.VMEM((elements, LANES), f32),
            pltpu.VMEM((elements, LANES), f32),
            pltpu.VMEM((elements, LANES), f32),
            pltpu.VMEM((elements, LANES), f32),
            pltpu.VMEM((2, 4, border, LANES), f32),
            pltpu.VMEM((2, 4, border, LANES), f32),
            pltpu.VMEM(pairs.shape, jnp.int32),
            pltpu.VMEM((1, LANES), f32),
            pltpu.VMEM((devices, 1, LANES), f32),
            pltpu.VMEM((rows, LANES), f32),
            pltpu.VMEM((devices, rows, LANES), f32),
            pltpu.SemaphoreType.DMA((9,)),
            pltpu.SemaphoreType.DMA((2, 4)),
            pltpu.SemaphoreType.DMA((2, 4)),
            pltpu.SemaphoreType.DMA((2,)),
            pltpu.SemaphoreType.DMA((2,)),
        ],
        compiler_params=pltpu.CompilerParams(collective_id=0, has_side_effects=True),
        name="arnoldi",
    )(restart_coeffs, old_basis, geometry, orientation, forward, backward, coef, pairs)
    return held


def solution(mesh):
    in_specs = (
        P(None, ("wide", "narrow"), None),
        P(),
        P(None, ("wide", "narrow"), None),
        P(None, ("wide", "narrow")),
    )
    out_specs = (P(None, ("wide", "narrow"), None), P())
    return jax.shard_map(
        functools.partial(on_device, mesh.shape["wide"], mesh.shape["narrow"]),
        mesh=mesh,
        in_specs=in_specs,
        out_specs=out_specs,
        check_vma=False,
    )
```

```python
import functools

import jax
import jax.numpy as jnp
import numpy as np
from jax import lax
from jax.experimental import pallas as pl
from jax.experimental.pallas import tpu as pltpu
from jax.sharding import PartitionSpec as P

NP = 8
EX = 4
EY = 4
EZ = 4
LANES = 128
FACE = NP * NP
MESH = pl.DeviceIdType.MESH
highest = lax.Precision.HIGHEST
epsilon = 1e-06


def legendre_columns(nodes, degree):
    columns = [nodes * 0.0 + 1.0, nodes * 1.0]
    for order in range(2, degree + 1):
        columns.append(
            ((2 * order - 1) * nodes * columns[order - 1] - (order - 1) * columns[order - 2])
            / order
        )
    return columns


def gll_derivative(extent):
    degree = extent - 1
    nodes = np.cos(np.pi * np.arange(extent) / degree)
    for sweep in range(100):
        columns = legendre_columns(nodes, degree)
        nodes = nodes - (nodes * columns[degree] - columns[degree - 1]) / (extent * columns[degree])
    gll_nodes = nodes[::-1] * 1.0
    values = legendre_columns(gll_nodes, degree)[degree]
    matrix = np.zeros((extent, extent))
    for row_idx in range(extent):
        for col_idx in range(extent):
            if row_idx != col_idx:
                matrix[row_idx, col_idx] = values[row_idx] / (
                    values[col_idx] * (gll_nodes[row_idx] - gll_nodes[col_idx])
                )
    matrix[0, 0] = -degree * (degree + 1) / 4.0
    matrix[extent - 1, extent - 1] = degree * (degree + 1) / 4.0
    return matrix


def tables():
    matrix = gll_derivative(NP)
    identity = np.eye(NP)
    pair = np.eye(2)
    along_y = np.kron(pair, np.kron(matrix, identity))
    along_z = np.kron(pair, np.kron(identity, matrix))
    forward = np.concatenate([along_y.T, along_z.T], axis=1)
    backward = np.concatenate([along_y, along_z], axis=0)
    tiles = NP // 2
    coef = np.zeros((2, tiles, tiles, 2, LANES))
    for way, table in enumerate((matrix, matrix.T)):
        for out_tile in range(tiles):
            for in_tile in range(tiles):
                for half in range(2):
                    lanes = slice(half * FACE, (half + 1) * FACE)
                    row = 2 * out_tile + half
                    coef[way, out_tile, in_tile, 0, lanes] = table[row, 2 * in_tile + half]
                    coef[way, out_tile, in_tile, 1, lanes] = table[row, 2 * in_tile + 1 - half]
    return (
        jnp.asarray(forward, jnp.float32),
        jnp.asarray(backward, jnp.float32),
        jnp.asarray(coef.reshape(-1, LANES), jnp.float32),
    )


def pair_rows(kept):
    count = kept + 2
    listed = [(at, kept + 1) for at in range(count)]
    listed += [(at, kept) for at in range(kept + 1)]
    block = 4
    for left in range(0, kept, block):
        for right in range(left, kept, block):
            for one in range(left, left + block):
                for two in range(max(right, one), right + block):
                    listed.append((one, two))
    return -(-len(listed) // LANES), listed


def take_lanes(values, index):
    return jnp.take_along_axis(values, index, axis=1, mode="promise_in_bounds")


def rotated(row, col, code):
    row = row ^ (7 * (code & 1))
    col = col ^ (7 * ((code >> 1) & 1))
    return jnp.where((code & 4) != 0, col * NP + row, row * NP + col)


def kernel(
    n_wide,
    n_narrow,
    coeffs,
    basis_hbm,
    geom_hbm,
    orient,
    forward_hbm,
    backward_hbm,
    coef_hbm,
    pairs_hbm,
    out,
    hess,
    basis,
    geom,
    forward,
    backward,
    coef,
    index,
    orient_pad,
    image,
    first,
    face_y,
    face_z,
    halo_y,
    halo_z,
    outbox,
    inbox,
    pairs,
    row_out,
    row_in,
    pair_out,
    pair_in,
    load_sem,
    halo_send,
    halo_recv,
    row_send,
    row_recv,
):
    wide = lax.axis_index("wide")
    narrow = lax.axis_index("narrow")
    devices = n_wide * n_narrow
    me = wide * n_narrow + narrow
    kept, elements, points = basis.shape
    tiles = points // LANES
    total = float(elements * points * devices)

    def load(source, target, slot):
        return pltpu.make_async_copy(source, target, load_sem.at[slot])

    chunk = kept // 4
    loads = [
        load(basis_hbm.at[pl.ds(part * chunk, chunk)], basis.at[pl.ds(part * chunk, chunk)], part)
        for part in range(4)
    ]
    loads += [
        load(forward_hbm, forward, 4),
        load(geom_hbm, geom, 5),
        load(backward_hbm, backward, 6),
        load(coef_hbm, coef, 7),
        load(pairs_hbm, pairs, 8),
    ]
    for copy in loads:
        copy.start()

    messages = ((row_out, row_in), (pair_out, pair_in))
    inbox[...] = jnp.zeros_like(inbox)

    def peer(step):
        if devices & (devices - 1):
            other = lax.rem(me + step, devices)
        else:
            other = me
            for bit in range(devices.bit_length() - 1):
                if step >> bit & 1:
                    other = other + (1 - 2 * lax.rem(me // 2**bit, 2)) * 2**bit
        return (other // n_narrow, lax.rem(other, n_narrow))

    def each_peer(act):
        if devices <= 64:
            for step in range(devices - 1, 0, -1):
                act(peer(step))
        else:

            def body(step, carry):
                other = lax.rem(me + step, devices)
                act((other // n_narrow, lax.rem(other, n_narrow)))
                return carry

            lax.fori_loop(1, devices, body, 0)

    barrier = pltpu.get_barrier_semaphore()

    def greet(where):
        pl.semaphore_signal(barrier, inc=1, device_id=where, device_id_type=MESH)

    each_peer(greet)

    lane = lax.broadcasted_iota(jnp.int32, (elements, LANES), 1)
    line = lax.broadcasted_iota(jnp.int32, (elements, LANES), 0)
    low_half = lane < FACE
    half = lane // FACE
    mid = (lane // NP) % NP
    fast = lane % NP
    row_y = (line // EZ) % EY
    row_z = line % EZ
    at_y = (mid == 0) | (mid == NP - 1)
    at_z = (fast == 0) | (fast == NP - 1)

    orient_pad[...] = jnp.zeros_like(orient_pad)
    orient_pad[pl.ds(0, 6), pl.ds(0, elements)] = orient[...]
    codes = jnp.transpose(orient_pad[...])[:elements]
    code = [jnp.broadcast_to(codes[:, f : f + 1], (elements, LANES)) for f in range(6)]
    code_x = jnp.where(low_half, code[0], code[1])
    index[2 * tiles] = rotated(mid, fast, code_x) + jnp.where(low_half, FACE, 0)
    code_y = jnp.where(mid == 0, code[2], code[3])
    code_z = jnp.where(fast == 0, code[4], code[5])
    for tile in range(tiles):
        first_pos = 2 * tile + half
        index[tile] = rotated(first_pos, fast, code_y) + jnp.where(mid == 0, FACE, 0)
        index[tiles + tile] = rotated(first_pos, mid, code_z) + jnp.where(fast == 0, FACE, 0)

    pick_y = (mid % 2) * FACE + half * (FACE - NP) + fast
    pick_z = (mid % 2) * FACE + fast * NP + half * (NP - 1)
    source_tile = mid // 2

    def tile_of(values, tile):
        return values[:, tile * LANES : (tile + 1) * LANES]

    def swap(values):
        return pltpu.roll(values, FACE, axis=1)

    def along_x(parts, way):
        swapped = [swap(part) for part in parts]
        outs = []
        for out_tile in range(tiles):
            acc = None
            for in_tile in range(tiles):
                at = ((way * tiles + out_tile) * tiles + in_tile) * 2
                term = (
                    coef[pl.ds(at, 1), :] * parts[in_tile]
                    + coef[pl.ds(at + 1, 1), :] * swapped[in_tile]
                )
                acc = term if acc is None else acc + term
            outs.append(acc)
        return outs

    def local(parts):
        stacked = jnp.concatenate(parts, axis=0)
        grads = jnp.dot(
            stacked, forward[...], precision=highest, preferred_element_type=jnp.float32
        )
        geom_y = jnp.concatenate([geom[1, :, pl.ds(t * LANES, LANES)] for t in range(tiles)], axis=0)
        geom_z = jnp.concatenate([geom[2, :, pl.ds(t * LANES, LANES)] for t in range(tiles)], axis=0)
        flux = jnp.concatenate([grads[:, :LANES] * geom_y, grads[:, LANES:] * geom_z], axis=1)
        back = jnp.dot(
            flux, backward[...], precision=highest, preferred_element_type=jnp.float32
        )
        grad_x = along_x(parts, 0)
        flux_x = [grad_x[t] * geom[0, :, pl.ds(t * LANES, LANES)] for t in range(tiles)]
        back_x = along_x(flux_x, 1)
        return [
            back[t * elements : (t + 1) * elements]
            + back_x[t]
            + geom[3, :, pl.ds(t * LANES, LANES)] * parts[t]
            for t in range(tiles)
        ]

    def faces(parts, pick):
        found = take_lanes(parts[0], pick)
        for tile in range(1, tiles):
            found = jnp.where(source_tile == tile, take_lanes(parts[tile], pick), found)
        return found

    has = (narrow > 0, narrow < n_narrow - 1, wide > 0, wide < n_wide - 1)
    where_to = ((wide, narrow - 1), (wide, narrow + 1), (wide - 1, narrow), (wide + 1, narrow))

    def face_copy(step, side):
        return pltpu.make_async_remote_copy(
            src_ref=outbox.at[step, side],
            dst_ref=inbox.at[step, side ^ 1],
            send_sem=halo_send.at[step, side],
            recv_sem=halo_recv.at[step, side ^ 1],
            device_id=where_to[side],
            device_id_type=MESH,
        )

    def face_arrival(step, side):
        return pltpu.make_async_copy(
            inbox.at[step, side], inbox.at[step, side], halo_recv.at[step, side]
        )

    def operate(parts, step, ready, beside=lambda: None):
        result = local(parts)
        def send_faces(sides):
            for side in sides:

                @pl.when(has[side])
                def _():
                    face_copy(step, side).start()

        found_z = faces(result, pick_z)
        face_z[...] = found_z
        outbox[step, 2] = face_z[pl.ds(0, EX * EY, stride=EZ), :]
        outbox[step, 3] = face_z[pl.ds(EZ - 1, EX * EY, stride=EZ), :]
        ready()
        send_faces((2, 3))
        found_y = faces(result, pick_y)
        face_y[...] = found_y
        for ex in range(EX):
            outbox[step, 0, pl.ds(ex * EZ, EZ), :] = face_y[pl.ds(ex * EY * EZ, EZ), :]
            outbox[step, 1, pl.ds(ex * EZ, EZ), :] = face_y[pl.ds(ex * EY * EZ + (EY - 1) * EZ, EZ), :]
        send_faces((0, 1))

        face_x = jnp.where(low_half, result[0], result[tiles - 1])
        width = EY * EZ
        blank = jnp.zeros((width, LANES), jnp.float32)
        in_x = jnp.where(
            low_half,
            jnp.concatenate([face_x[width:], blank], axis=0),
            jnp.concatenate([blank, face_x[: elements - width]], axis=0),
        )
        in_y = jnp.where(
            low_half, pltpu.roll(found_y, elements - EZ, axis=0), pltpu.roll(found_y, EZ, axis=0)
        )
        in_z = jnp.where(
            low_half, pltpu.roll(found_z, elements - 1, axis=0), pltpu.roll(found_z, 1, axis=0)
        )
        got_x = take_lanes(in_x, index[2 * tiles])
        result[0] = result[0] + jnp.where(low_half, got_x, 0.0)
        result[tiles - 1] = result[tiles - 1] + jnp.where(low_half, 0.0, got_x)

        beside()

        def await_faces(sides):
            for side in sides:

                @pl.when(has[side])
                def _():
                    face_arrival(step, side).wait()

        await_faces((0, 1))
        for ex in range(EX):
            halo_y[pl.ds(ex * EY * EZ, EZ), :] = inbox[step, 0, pl.ds(ex * EZ, EZ), :]
            halo_y[pl.ds(ex * EY * EZ + (EY - 1) * EZ, EZ), :] = inbox[step, 1, pl.ds(ex * EZ, EZ), :]
        edge_y = row_y == jnp.where(low_half, EY - 1, 0)
        in_y = jnp.where(edge_y, halo_y[...], in_y)
        for t in range(tiles):
            result[t] = result[t] + jnp.where(at_y, take_lanes(in_y, index[t]), 0.0)
            image[:, pl.ds(t * LANES, LANES)] = result[t]

        await_faces((2, 3))
        halo_z[pl.ds(0, EX * EY, stride=EZ), :] = inbox[step, 2]
        halo_z[pl.ds(EZ - 1, EX * EY, stride=EZ), :] = inbox[step, 3]
        edge_z = row_z == jnp.where(low_half, EZ - 1, 0)
        in_z = jnp.where(edge_z, halo_z[...], in_z)
        return [
            image[:, pl.ds(t * LANES, LANES)]
            + jnp.where(at_z, take_lanes(in_z, index[tiles + t]), 0.0)
            for t in range(tiles)
        ]

    def folded(values):
        acc = tile_of(values, 0)
        for tile in range(1, tiles):
            acc = acc + tile_of(values, tile)
        return jnp.sum(acc.reshape(elements // 8, 8, LANES), axis=0)

    def to_row(partials, begin=0):
        count = -(-len(partials) // 8) * 8
        rows = [jnp.sum(part, axis=0, keepdims=True) for part in partials]
        rows += [jnp.zeros((1, LANES), jnp.float32)] * (count - len(rows))
        block = jnp.concatenate(rows, axis=0)
        sums = jnp.sum(block, axis=1, keepdims=True)
        place = lax.broadcasted_iota(jnp.int32, (count, LANES), 0) + begin == lax.broadcasted_iota(
            jnp.int32, (count, LANES), 1
        )
        return jnp.sum(jnp.where(place, sums, 0.0), axis=0, keepdims=True)

    def all_sum(block, phase, beside):
        outgoing, incoming = messages[phase]
        outgoing[...] = block
        incoming[pl.ds(me, 1)] = block.reshape((1,) + block.shape)

        def send(where):
            pltpu.make_async_remote_copy(
                src_ref=outgoing,
                dst_ref=incoming.at[me],
                send_sem=row_send.at[phase],
                recv_sem=row_recv.at[phase],
                device_id=where,
                device_id_type=MESH,
            ).start()

        each_peer(send)
        result = beside()
        span = incoming.at[pl.ds(0, devices - 1)]
        pltpu.make_async_copy(span, span, row_recv.at[phase]).wait()
        return jnp.sum(incoming[...], axis=0), result

    def weight(row, at):
        return row[:, at : at + 1]

    start = None
    for part in range(4):
        loads[part].wait()
        for at in range(part * chunk, (part + 1) * chunk):
            term = coeffs[at] * basis[at]
            start = term if start is None else start + term
    for copy in loads[4:]:
        copy.wait()

    def greeted():
        pl.semaphore_wait(barrier, devices - 1)

    image_parts = operate([tile_of(start, t) for t in range(tiles)], 0, greeted)
    for t in range(tiles):
        image[:, pl.ds(t * LANES, LANES)] = image_parts[t]
    rows, listed = pair_rows(kept)
    fresh = 2 * kept + 3

    def gram():
        partials = []
        block = 4
        for left in range(0, kept, block):
            for right in range(left, kept, block):
                wanted = [
                    (one, two)
                    for one in range(left, left + block)
                    for two in range(max(right, one), right + block)
                ]

                def body(step, carry):
                    base = pl.multiple_of(step * 8, 8)
                    carry = list(carry)
                    for tile in range(tiles):
                        at = (pl.ds(base, 8), pl.ds(tile * LANES, LANES))
                        ones = [basis[(left + m,) + at] for m in range(block)]
                        twos = ones if left == right else [
                            basis[(right + m,) + at] for m in range(block)
                        ]
                        for spot, (one, two) in enumerate(wanted):
                            carry[spot] = carry[spot] + ones[one - left] * twos[two - right]
                    return tuple(carry)

                zero = jnp.zeros((8, LANES), jnp.float32)
                partials += list(
                    lax.fori_loop(0, elements // 8, body, (zero,) * len(wanted))
                )
        gram_rows = []
        for begin in range(0, rows * LANES, LANES):
            lo = max(begin, fresh)
            here = partials[lo - fresh : begin + LANES - fresh]
            row = to_row(here, lo - begin) if here else jnp.zeros((1, LANES), jnp.float32)
            gram_rows.append(row)
        return gram_rows

    row = to_row([folded(basis[at] * image[...]) for at in range(kept)])
    sums, gram_part = all_sum(row, 0, gram)
    proj_one = sums / total
    acc = image[...]
    for at in range(kept):
        acc = acc - weight(proj_one, at) * basis[at]
    first[...] = acc

    with_first = []

    def project_first():
        with_first.extend(
            [folded(basis[at] * first[...]) for at in range(kept)]
            + [folded(first[...] * first[...])]
        )

    image_parts = operate(
        [first[:, pl.ds(t * LANES, LANES)] for t in range(tiles)], 1, lambda: None, project_first
    )
    for t in range(tiles):
        image[:, pl.ds(t * LANES, LANES)] = image_parts[t]
    row = to_row(
        [folded(basis[at] * image[...]) for at in range(kept)]
        + [folded(first[...] * image[...]), folded(image[...] * image[...])]
        + with_first
    )
    block = jnp.concatenate([gram_part[0] + row] + gram_part[1:], axis=0)
    sums, _ = all_sum(block, 1, lambda: None)
    sums = sums / total
    along = sums[0:1]
    norm_one = jnp.sqrt(weight(along, fresh - 1) + epsilon)
    scale_one = 1.0 / norm_one
    proj_two = along * scale_one
    self_two = weight(along, kept) * scale_one * scale_one

    spot = lax.broadcasted_iota(jnp.int32, (8, LANES), 1)
    factor = jnp.broadcast_to(along, (8, LANES))
    factor = jnp.where(spot < kept, -factor, 0.0)
    factor = jnp.where(spot == kept, -self_two, factor)
    factor = jnp.where(spot == kept + 1, 1.0, factor)
    square = jnp.zeros((1, LANES), jnp.float32)
    for at in range(rows):
        left = jnp.broadcast_to(pairs[pl.ds(at, 1), :], (8, LANES))
        right = jnp.broadcast_to(pairs[pl.ds(rows + at, 1), :], (8, LANES))
        product = take_lanes(factor, left) * take_lanes(factor, right)
        product = jnp.where(left == right, product, 2.0 * product)
        used = spot + at * LANES < len(listed)
        square = square + jnp.where(used, product * sums[at : at + 1], 0.0)[0:1]
    square = jnp.maximum(jnp.sum(square, axis=1, keepdims=True), 0.0) * (scale_one * scale_one)
    norm_two = jnp.sqrt(square + epsilon)

    acc = image[...] - (self_two * first[...])
    for at in range(kept):
        acc = acc - weight(along, at) * basis[at]
    out[0] = first[...] * scale_one
    out[1] = acc * (scale_one / norm_two)

    spot = lax.broadcasted_iota(jnp.int32, (1, LANES), 1)
    row_first = jnp.where(spot < kept, proj_one, jnp.where(spot == kept, norm_one, 0.0))
    row_second = jnp.where(spot < kept, proj_two, jnp.where(spot == kept, self_two, norm_two))
    hess[pl.ds(0, 1), :] = row_first[:, : kept + 2]
    hess[pl.ds(1, 1), :] = row_second[:, : kept + 2]

    for step in range(2):
        for side in range(4):

            @pl.when(has[side])
            def _():
                face_copy(step, side).wait_send()

    for phase in range(2):
        span = messages[phase][1].at[pl.ds(0, devices - 1)]
        pltpu.make_async_copy(span, span, row_send.at[phase]).wait()


def on_device(n_wide, n_narrow, old_basis, restart_coeffs, geometry, orientation):
    kept, elements, points = old_basis.shape
    tiles = points // LANES
    devices = n_wide * n_narrow
    forward, backward, coef = tables()
    rows, listed = pair_rows(kept)
    pairs = np.zeros((2 * rows, LANES), np.int32)
    for at, (left, right) in enumerate(listed):
        pairs[at // LANES, at % LANES] = left
        pairs[rows + at // LANES, at % LANES] = right
    pairs = jnp.asarray(pairs)
    anywhere = pl.BlockSpec(memory_space=pl.ANY)
    vmem = pl.BlockSpec(memory_space=pltpu.VMEM)
    f32 = jnp.float32
    border = EX * EY
    shapes = ((2, elements, points), (2, kept + 2))
    held = pl.pallas_call(
        functools.partial(kernel, n_wide, n_narrow),
        out_shape=tuple(pltpu.VMEM(shape, f32) for shape in shapes),
        in_specs=[
            pl.BlockSpec(memory_space=pltpu.SMEM),
            anywhere,
            anywhere,
            vmem,
            anywhere,
            anywhere,
            anywhere,
            anywhere,
        ],
        out_specs=(vmem, vmem),
        scratch_shapes=[
            pltpu.VMEM(old_basis.shape, f32),
            pltpu.VMEM(geometry.shape, f32),
            pltpu.VMEM(forward.shape, f32),
            pltpu.VMEM(backward.shape, f32),
            pltpu.VMEM(coef.shape, f32),
            pltpu.VMEM((2 * tiles + 1, elements, LANES), jnp.int32),
            pltpu.VMEM((8, LANES), jnp.int32),
            pltpu.VMEM((elements, points), f32),
            pltpu.VMEM((elements, points), f32),
            pltpu.VMEM((elements, LANES), f32),
            pltpu.VMEM((elements, LANES), f32),
            pltpu.VMEM((elements, LANES), f32),
            pltpu.VMEM((elements, LANES), f32),
            pltpu.VMEM((2, 4, border, LANES), f32),
            pltpu.VMEM((2, 4, border, LANES), f32),
            pltpu.VMEM(pairs.shape, jnp.int32),
            pltpu.VMEM((1, LANES), f32),
            pltpu.VMEM((devices, 1, LANES), f32),
            pltpu.VMEM((rows, LANES), f32),
            pltpu.VMEM((devices, rows, LANES), f32),
            pltpu.SemaphoreType.DMA((9,)),
            pltpu.SemaphoreType.DMA((2, 4)),
            pltpu.SemaphoreType.DMA((2, 4)),
            pltpu.SemaphoreType.DMA((2,)),
            pltpu.SemaphoreType.DMA((2,)),
        ],
        compiler_params=pltpu.CompilerParams(collective_id=0, has_side_effects=True),
        name="arnoldi",
    )(restart_coeffs, old_basis, geometry, orientation, forward, backward, coef, pairs)
    return held


def solution(mesh):
    in_specs = (
        P(None, ("wide", "narrow"), None),
        P(),
        P(None, ("wide", "narrow"), None),
        P(None, ("wide", "narrow")),
    )
    out_specs = (P(None, ("wide", "narrow"), None), P())
    return jax.shard_map(
        functools.partial(on_device, mesh.shape["wide"], mesh.shape["narrow"]),
        mesh=mesh,
        in_specs=in_specs,
        out_specs=out_specs,
        check_vma=False,
    )
```
